32 devices in a mesh: groups: 2 (over x), frame: 16 (over z, y, core).
Axes of the slice: x: 2, y: 2, z: 4, core: 2. Of those that a mesh axis runs over, the one named last changes fastest.
Arguments:
- latents: bfloat16 [128, 2, 64, 320], P(('groups', 'frame')), parts along dimension 0, may hold values from -6 to 6
- norm_gain: float32 [320], replicated, may hold values from 0.1 to 1.9
- w_qkv: bfloat16 [320, 960], replicated, may hold values from -0.3125 to 0.3125
- w_out: bfloat16 [320, 320], replicated, may hold values from -0.3125 to 0.3125
- gn_gain: float32 [2, 320], replicated, may hold values from 0.1 to 1.9
- conv_one: bfloat16 [3, 3, 320, 320], replicated, may hold values from -0.109375 to 0.109375
- conv_two: bfloat16 [3, 3, 320, 320], replicated, may hold values from -0.109375 to 0.109375
- step_embed: float32 [320], replicated, may hold values from -4 to 4
- offsets: int32 [32], P('groups'), parts along dimension 0, may hold values from 0 to 3
- numerators: int32 [16], replicated, may hold values from 1 to 16
Outputs:
- result: bfloat16 [128, 2, 64, 320], P(('groups', 'frame')), parts along dimension 0
The draws below stay inside these ranges and needn't reach their ends.
There are 2 independent parts, one for each index of `groups`. The reference program is written for one: setup_inputs(seed, part) draws one part's arguments, and reference() takes and returns one part's arrays. A program takes and returns all parts, laid end to end along the dimension named above; an argument that names none is the same for every part. Nothing has to cross between parts.
All inputs are finite; a program needn't handle non-finite values.
Results may differ from the reference program's by a relative error of at most 0.009.
Values may be sent and summed in bfloat16 or wider, within the bound.
A program may use at most 64 MiB of HBM per device.

```python
import jax
import jax.numpy as jnp
from jax import lax

C = 320
HEADS = 5
HEAD_DIM = 64
NORM_GROUPS = 32
BLOCK = 4
WINDOW = 16
ROWS = 2
COLS = 64
BLOCKS = 16
FRAMES = 64


def place_ends(result, own_key, low, high):
    dims = result.shape
    place = [jax.random.randint(jax.random.fold_in(own_key, axis), (), 0, dims[axis]) for axis in range(len(dims))]
    result = result.at[tuple(place)].set(low)
    longest = dims.index(max(dims))
    place[longest] = (place[longest] + 1) % dims[longest]
    return result.at[tuple(place)].set(high)


def block_scale(stream_key, dims, shards, low, high):
    level, own = 1.0, jax.random.fold_in(stream_key, 6)
    for axis_at, blocks in shards:
        draws = jnp.exp(jax.random.uniform(jax.random.fold_in(own, axis_at), (blocks,), jnp.float32, low / len(shards), high / len(shards)))
        level = level * jnp.repeat(draws, dims[axis_at] // blocks).reshape([-1 if axis == axis_at else 1 for axis in range(len(dims))])
    return level


def bell_draw(own_key, extent, width, reach, shards=(), held_as=jnp.bfloat16):
    result = jax.random.normal(own_key, extent, jnp.float32) * width
    if len(shards) > 0:
        result = block_scale(own_key, extent, shards, -0.22, 0.18) * result
    return jnp.clip(result, min=-reach, max=reach).astype(held_as)


def setup_inputs(seed: int = 0, part: int = 0) -> dict:
    key_of = jax.random.split(jax.random.key(seed), 11)
    part_splits = jax.random.split(jax.random.fold_in(key_of[10], part), 11)
    return {
        "latents": bell_draw(part_splits[0], (FRAMES, ROWS, COLS, C), 1.0, 6.0, ((0, 16),)),
        "norm_gain": jnp.clip(1.0 + 0.18 * jax.random.normal(key_of[1], (C,), jnp.float32), 0.1, 1.9),
        "w_qkv": bell_draw(key_of[2], (C, 3 * C), C ** -0.5, 0.3125),
        "w_out": bell_draw(key_of[3], (C, C), C ** -0.5, 0.3125),
        "gn_gain": jnp.clip(1.0 + 0.18 * jax.random.normal(key_of[4], (2, C), jnp.float32), 0.1, 1.9),
        "conv_one": bell_draw(key_of[5], (3, 3, C, C), (9 * C) ** -0.5, 0.109375),
        "conv_two": bell_draw(key_of[6], (3, 3, C, C), (9 * C) ** -0.5, 0.109375),
        "step_embed": bell_draw(key_of[7], (C,), 1.0, 4.0, (), jnp.float32),
        "offsets": place_ends(jax.random.randint(part_splits[8], (BLOCKS,), 0, BLOCK), jax.random.fold_in(part_splits[8], 1), 0, BLOCK - 1).astype(jnp.int32),
        "numerators": place_ends(jax.random.randint(key_of[9], (WINDOW,), 1, 17), jax.random.fold_in(key_of[9], 1), 1, 16).astype(jnp.int32),
    }


def layer_project(frames, norm_gain, w_qkv):
    channels = frames.shape[-1]
    values32 = frames.astype(jnp.float32)
    average = lax.optimization_barrier(jnp.mean(values32, axis=-1, keepdims=True))
    centered = values32 - average
    variance = lax.optimization_barrier(jnp.mean(centered * centered, axis=-1, keepdims=True))
    normed = (centered * lax.rsqrt(variance + 1e-05) * norm_gain).astype(jnp.bfloat16)
    qkv = jnp.dot(normed.reshape(-1, channels), w_qkv, preferred_element_type=jnp.float32).astype(jnp.bfloat16)
    return qkv.reshape(frames.shape[0], -1, 3 * channels)

def window_attend(window, numer_f):
    frame_count, pos_count, triple = window.shape
    channels = triple // 3
    queries = window[..., :channels].reshape(frame_count, pos_count, HEADS, HEAD_DIM).astype(jnp.float32)
    keys = window[..., channels:2 * channels].reshape(frame_count, pos_count, HEADS, HEAD_DIM).astype(jnp.float32)
    values = window[..., 2 * channels:].reshape(frame_count, pos_count, HEADS, HEAD_DIM).astype(jnp.float32)
    scores = jnp.einsum('jphd,kphd->phjk', queries, keys) / jnp.sqrt(jnp.float32(HEAD_DIM))
    highest = lax.optimization_barrier(jnp.max(scores, axis=-1, keepdims=True))
    expos = jnp.exp(scores - highest)
    probs = (expos / lax.optimization_barrier(jnp.sum(expos, axis=-1, keepdims=True))).astype(jnp.bfloat16)
    attended = jnp.einsum('phjk,kphd->jphd', probs.astype(jnp.float32), values).reshape(frame_count, pos_count, channels)
    return (attended * numer_f[:, None, None]).astype(jnp.bfloat16)

def group_act(tensor, gain):
    shape = tensor.shape
    grouped = tensor.reshape(shape[0], shape[1], shape[2], NORM_GROUPS, shape[3] // NORM_GROUPS)
    average = lax.optimization_barrier(jnp.mean(grouped, axis=(1, 2, 4), keepdims=True))
    centered = grouped - average
    variance = lax.optimization_barrier(jnp.mean(centered * centered, axis=(1, 2, 4), keepdims=True))
    normed = (centered * lax.rsqrt(variance + 1e-05)).reshape(shape) * gain
    return jax.nn.silu(normed).astype(jnp.bfloat16)

def conv_three(tensor, kernel):
    return lax.conv_general_dilated(tensor.astype(jnp.float32), kernel.astype(jnp.float32), (1, 1), 'SAME', dimension_numbers=('NHWC', 'HWIO', 'NHWC'), preferred_element_type=jnp.float32)

def reference(latents, norm_gain, w_qkv, w_out, gn_gain, conv_one, conv_two, step_embed, offsets, numerators):
    channels = latents.shape[-1]
    qkv = layer_project(latents, norm_gain, w_qkv)
    numer_f = numerators.astype(jnp.float32)
    steps_in = jnp.arange(WINDOW, dtype=jnp.int32)

    def add_window(totals, window_id):
        frame_index = ((BLOCK * window_id + offsets[window_id] + steps_in) % FRAMES).astype(jnp.int32)
        weighted = window_attend(qkv[frame_index], numer_f)
        return (totals.at[frame_index].add(weighted.astype(jnp.float32)), None)
    empty = jnp.zeros((FRAMES, qkv.shape[1], channels), jnp.float32)
    totals, unused = lax.scan(add_window, empty, jnp.arange(BLOCKS, dtype=jnp.int32))
    all_index = ((BLOCK * jnp.arange(BLOCKS, dtype=jnp.int32)[:, None] + offsets[:, None] + steps_in[None, :]) % FRAMES).astype(jnp.int32)
    denominator = jnp.zeros((FRAMES,), jnp.float32).at[all_index.reshape(-1)].add(jnp.tile(numer_f, BLOCKS))
    combined = (totals / denominator[:, None, None]).astype(jnp.bfloat16)
    projected = jnp.dot(combined.reshape(-1, channels), w_out, preferred_element_type=jnp.float32).reshape(latents.shape)
    hidden = (latents.astype(jnp.float32) + projected).astype(jnp.bfloat16)
    first_act = group_act(hidden.astype(jnp.float32), gn_gain[0])
    middle = conv_three(first_act, conv_one) + step_embed
    second_act = group_act(middle, gn_gain[1])
    return (hidden.astype(jnp.float32) + conv_three(second_act, conv_two)).astype(jnp.bfloat16)
```

```python
import functools

import jax
import jax.numpy as jnp
from jax import lax
from jax.experimental import pallas as pl
from jax.experimental.pallas import tpu as pltpu
from jax.sharding import PartitionSpec as P

HEADS = 5
HEAD_DIM = 64
NORM_GROUPS = 32
WINDOW = 16
LANES = 128
EPS = 1e-05
FAR = -1e30
F32 = jnp.float32
BF16 = jnp.bfloat16
MESH = pl.DeviceIdType.MESH
VMEM = pl.BlockSpec(memory_space=pltpu.VMEM)
SMEM = pl.BlockSpec(memory_space=pltpu.SMEM)
ANY = pl.BlockSpec(memory_space=pl.ANY)


def meet(count):
    me = lax.axis_index("frame")
    barrier = pltpu.get_barrier_semaphore()
    for step in range(1, count):
        pl.semaphore_signal(
            barrier, inc=1, device_id={"frame": lax.rem(me + step, count)}, device_id_type=MESH
        )
    pl.semaphore_wait(barrier, count - 1)


def exchange(count, source, target, send_sem, recv_sem, own_sem):
    me = lax.axis_index("frame")
    copies = []
    for step in range(1, count):
        peer = lax.rem(me + step, count)
        copy = pltpu.make_async_remote_copy(
            src_ref=source(peer),
            dst_ref=target(me),
            send_sem=send_sem.at[step],
            recv_sem=recv_sem.at[step],
            device_id={"frame": peer},
            device_id_type=MESH,
        )
        copy.start()
        copies.append(copy)
    own = pltpu.make_async_copy(source(me), target(me), own_sem)
    own.start()
    own.wait()
    for copy in copies:
        copy.wait()


def spread_kernel(count, x_ref, y_ref, send_sem, recv_sem, own_sem):
    meet(count)
    exchange(count, lambda i: x_ref.at[:, i], lambda i: y_ref.at[i], send_sem, recv_sem, own_sem)


def gather_kernel(count, y_ref, z_ref, send_sem, recv_sem, own_sem):
    meet(count)
    exchange(count, lambda i: y_ref.at[i], lambda i: z_ref.at[:, i], send_sem, recv_sem, own_sem)


def transfer(kernel, count, array, shape, identity):
    return pl.pallas_call(
        functools.partial(kernel, count),
        out_shape=jax.ShapeDtypeStruct(shape, array.dtype),
        in_specs=[ANY],
        out_specs=ANY,
        scratch_shapes=[
            pltpu.SemaphoreType.DMA((count,)),
            pltpu.SemaphoreType.DMA((count,)),
            pltpu.SemaphoreType.DMA,
        ],
        compiler_params=pltpu.CompilerParams(collective_id=identity, has_side_effects=True),
    )(array)


def mod_lane(shape, width, copies):
    lane = lax.broadcasted_iota(jnp.int32, shape, 1)
    out = lane
    for at in range(1, copies):
        out = jnp.where(lane >= at * width, lane - at * width, out)
    return out


def window_tables(frames, block, nblocks, copies, offsets_ref, numer_ref):
    reach = WINDOW // block
    width = copies * frames
    frame = mod_lane((1, width), frames, copies)
    rows = []
    for back in range(reach + 1):
        start = jnp.zeros((1, width), jnp.int32)
        for w in range(nblocks):
            first = block * ((w + back) % nblocks)
            start = jnp.where(
                (frame >= first) & (frame < first + block), block * w + offsets_ref[w], start
            )
        spot = frame - start
        spot = jnp.where(spot < 0, spot + frames, spot)
        spot = jnp.where(spot < 0, spot + frames, spot)
        numer = jnp.zeros((1, width), F32)
        for j in range(WINDOW):
            numer = jnp.where(spot == j, numer_ref[j].astype(F32), numer)
        rows.append((start, numer))
    total = rows[0][1]
    for _, numer in rows[1:]:
        total = total + numer
    key = lax.broadcasted_iota(jnp.int32, (frames, width), 0)
    tables = []
    for start, numer in rows:
        spot = key - start
        spot = jnp.where(spot < 0, spot + frames, spot)
        spot = jnp.where(spot < 0, spot + frames, spot)
        tables.append((jnp.where(spot < WINDOW, 0.0, FAR).astype(F32), numer / total))
    return tables


def attend(
    frames, cells, block, x_ref, gain_ref, w_ref, offsets_ref, numer_ref, out_ref,
    q_ref, k_ref, v_ref, comb_ref, bias_ref,
):
    channels = x_ref.shape[-1]
    rows = frames * cells
    nblocks = offsets_ref.shape[0]
    reach = WINDOW // block
    x = x_ref[...].astype(F32)
    average = jnp.mean(x, axis=-1, keepdims=True)
    centered = x - average
    variance = jnp.mean(centered * centered, axis=-1, keepdims=True)
    normed = (centered * lax.rsqrt(variance + EPS) * gain_ref[...]).astype(BF16)
    col = lax.broadcasted_iota(jnp.int32, (frames, rows), 1)
    row = lax.broadcasted_iota(jnp.int32, (frames, rows), 0)
    pick = jnp.concatenate(
        [jnp.where(col == row * cells + p, 1.0, 0.0).astype(BF16) for p in range(cells)], 0
    )
    normed = jnp.dot(pick, normed, preferred_element_type=F32).astype(BF16)
    for at, ref in enumerate((q_ref, k_ref, v_ref)):
        weight = w_ref[:, at * channels : (at + 1) * channels]
        ref[...] = jnp.dot(normed, weight, preferred_element_type=F32).astype(BF16)
    per = max(1, LANES // HEAD_DIM)
    tables = {}
    for first in range(0, HEADS, per):
        copies = min(per, HEADS - first)
        if copies not in tables:
            tables[copies] = None
    full = window_tables(frames, block, nblocks, per, offsets_ref, numer_ref)
    for back in range(reach + 1):
        bias_ref[back] = full[back][0]
    weights = [numer for _, numer in full]
    scale = HEAD_DIM**-0.5
    for p in range(cells):
        here = pl.ds(p * frames, frames)
        for first in range(0, HEADS, per):
            copies = min(per, HEADS - first)
            lanes = pl.ds(first * HEAD_DIM, copies * HEAD_DIM)
            q = q_ref[here, lanes]
            k = k_ref[here, lanes]
            v = v_ref[here, lanes]
            lane = lax.broadcasted_iota(jnp.int32, (frames, copies * HEAD_DIM), 1)
            spread = [
                jnp.where(
                    (lane >= h * HEAD_DIM) & (lane < (h + 1) * HEAD_DIM), q.astype(F32), 0.0
                ).astype(BF16)
                for h in range(copies)
            ]
            spread = jnp.concatenate(spread, 0) if copies > 1 else q
            scores = (
                lax.dot_general(
                    k, spread, (((1,), (1,)), ((), ())), preferred_element_type=F32
                )
                * scale
            )
            width = copies * frames
            total = jnp.zeros((frames, width), F32)
            for back in range(reach + 1):
                masked = scores + bias_ref[back, :, :width]
                expo = jnp.exp(masked - jnp.max(masked, axis=0, keepdims=True))
                level = weights[back][:, :width] / jnp.sum(expo, axis=0, keepdims=True)
                total = total + expo * level
            mixed = lax.dot_general(
                total.T.astype(BF16), v, (((1,), (0,)), ((), ())), preferred_element_type=F32
            )
            out = mixed[:frames]
            for h in range(1, copies):
                out = jnp.where(lane >= h * HEAD_DIM, mixed[h * frames : (h + 1) * frames], out)
            comb_ref[here, lanes] = out.astype(BF16)
    tall = lax.broadcasted_iota(jnp.int32, (rows, frames), 0)
    wide = lax.broadcasted_iota(jnp.int32, (rows, frames), 1)
    result = jnp.zeros((rows, channels), F32)
    for p in range(cells):
        back_pick = jnp.where(tall == wide * cells + p, 1.0, 0.0).astype(BF16)
        result = result + jnp.dot(
            back_pick, comb_ref[pl.ds(p * frames, frames), :], preferred_element_type=F32
        )
    out_ref[...] = result.astype(BF16)


def attention(x, gain, w_qkv, offsets, numerators, frames, cells, block):
    rows, channels = x.shape
    per = max(1, LANES // HEAD_DIM)
    return pl.pallas_call(
        functools.partial(attend, frames, cells, block),
        out_shape=jax.ShapeDtypeStruct(x.shape, BF16),
        in_specs=[VMEM, VMEM, VMEM, SMEM, SMEM],
        out_specs=VMEM,
        scratch_shapes=[pltpu.VMEM((rows, channels), BF16)] * 4
        + [pltpu.VMEM((WINDOW // block + 1, frames, per * frames), F32)],
        compiler_params=pltpu.CompilerParams(vmem_limit_bytes=60 * 2**20),
    )(x, gain, w_qkv, offsets, numerators)


def group_sum(sums):
    channels = sums.shape[-1]
    size = channels // NORM_GROUPS
    row = lax.broadcasted_iota(jnp.int32, (channels, channels), 0)
    col = lax.broadcasted_iota(jnp.int32, (channels, channels), 1)
    row_group = (row.astype(F32) * (1.0 / size) + 0.5 / size).astype(jnp.int32)
    col_group = (col.astype(F32) * (1.0 / size) + 0.5 / size).astype(jnp.int32)
    same = jnp.where(row_group == col_group, 1.0, 0.0).astype(F32)
    return jnp.dot(sums, same, preferred_element_type=F32, precision=lax.Precision.HIGHEST)


def group_act(tensor, gain):
    cells, channels = tensor[0].shape
    count = cells * (channels // NORM_GROUPS)
    sums = jnp.concatenate([jnp.sum(t, axis=0, keepdims=True) for t in tensor], 0)
    average = group_sum(sums) * (1.0 / count)
    centered = [t - average[i : i + 1] for i, t in enumerate(tensor)]
    squares = jnp.concatenate([jnp.sum(c * c, axis=0, keepdims=True) for c in centered], 0)
    factor = lax.rsqrt(group_sum(squares) * (1.0 / count) + EPS) * gain
    normed = [c * factor[i : i + 1] for i, c in enumerate(centered)]
    return [v / (1.0 + jnp.exp(-v)) for v in normed]


def conv_three(acts, conv_ref, tile_rows, tile_cols):
    count = len(acts)
    lines = []
    for r in range(tile_rows):
        line = jnp.concatenate([a[r * tile_cols : (r + 1) * tile_cols] for a in acts], 0)
        length = line.shape[0]
        at = jnp.concatenate(
            [lax.broadcasted_iota(jnp.int32, (tile_cols, line.shape[1]), 0)] * count, 0
        )
        before = jnp.where(at == 0, 0.0, pltpu.roll(line, 1, 0))
        after = jnp.where(at == tile_cols - 1, 0.0, pltpu.roll(line, length - 1, 0))
        lines.append([before.astype(BF16), line.astype(BF16), after.astype(BF16)])
    outs = []
    for r in range(tile_rows):
        total = None
        for s in range(max(0, r - 1), min(tile_rows, r + 2)):
            for x in range(3):
                term = jnp.dot(lines[s][x], conv_ref[s - r + 1, x], preferred_element_type=F32)
                total = term if total is None else total + term
        outs.append(total)
    return outs


def per_frame(lines, count, tile_cols):
    return [
        jnp.concatenate([line[i * tile_cols : (i + 1) * tile_cols] for line in lines], 0)
        for i in range(count)
    ]


def residual(
    block, tile_rows, tile_cols, x_ref, z_ref, w_out_ref, gn_ref, one_ref, two_ref, step_ref, out_ref
):
    cells = tile_rows * tile_cols
    projected = jnp.dot(z_ref[...], w_out_ref[...], preferred_element_type=F32)
    hidden = (x_ref[...].astype(F32) + projected).astype(BF16).astype(F32)
    hidden = [hidden[i * cells : (i + 1) * cells] for i in range(block)]
    acts = group_act(hidden, gn_ref[0:1])
    lines = conv_three(acts, one_ref, tile_rows, tile_cols)
    middle = per_frame([line + step_ref[...] for line in lines], block, tile_cols)
    acts = group_act(middle, gn_ref[1:2])
    lines = conv_three(acts, two_ref, tile_rows, tile_cols)
    moved = per_frame(lines, block, tile_cols)
    for i in range(block):
        out_ref[i * cells : (i + 1) * cells] = (hidden[i] + moved[i]).astype(BF16)


def resblock(x, z, w_out, gn_gain, conv_one, conv_two, step, block, tile_rows, tile_cols):
    return pl.pallas_call(
        functools.partial(residual, block, tile_rows, tile_cols),
        out_shape=jax.ShapeDtypeStruct(x.shape, BF16),
        in_specs=[VMEM] * 7,
        out_specs=VMEM,
        compiler_params=pltpu.CompilerParams(vmem_limit_bytes=60 * 2**20),
    )(x, z, w_out, gn_gain, conv_one, conv_two, step)


def body(
    latents, norm_gain, w_qkv, w_out, gn_gain, conv_one, conv_two, step_embed, offsets, numerators
):
    block, tile_rows, tile_cols, channels = latents.shape
    count = lax.axis_size("frame")
    cells = tile_rows * tile_cols // count
    frames = block * count
    split = latents.reshape(block, count, cells, channels)
    seen = transfer(spread_kernel, count, split, (count, block, cells, channels), 0)
    combined = attention(
        seen.reshape(frames * cells, channels),
        norm_gain.reshape(1, channels),
        w_qkv,
        offsets,
        numerators,
        frames,
        cells,
        block,
    )
    back = transfer(
        gather_kernel,
        count,
        combined.reshape(count, block, cells, channels),
        (block, count, cells, channels),
        1,
    )
    flat = (block * tile_rows * tile_cols, channels)
    result = resblock(
        latents.reshape(flat),
        back.reshape(flat),
        w_out,
        gn_gain,
        conv_one,
        conv_two,
        step_embed.reshape(1, channels),
        block,
        tile_rows,
        tile_cols,
    )
    return result.reshape(latents.shape)


def solution(mesh):
    return jax.shard_map(
        body,
        mesh=mesh,
        in_specs=(
            P(("groups", "frame"), None, None, None),
            P(),
            P(),
            P(),
            P(),
            P(),
            P(),
            P(),
            P("groups"),
            P(),
        ),
        out_specs=P(("groups", "frame"), None, None, None),
        check_vma=False,
    )
```

```python
import functools

import jax
import jax.numpy as jnp
from jax import lax
from jax.experimental import pallas as pl
from jax.experimental.pallas import tpu as pltpu
from jax.sharding import PartitionSpec as P

HEADS = 5
HEAD_DIM = 64
NORM_GROUPS = 32
WINDOW = 16
LANES = 128
EPS = 1e-05
FAR = -1e30
F32 = jnp.float32
BF16 = jnp.bfloat16
MESH = pl.DeviceIdType.MESH
VMEM = pl.BlockSpec(memory_space=pltpu.VMEM)
SMEM = pl.BlockSpec(memory_space=pltpu.SMEM)
ANY = pl.BlockSpec(memory_space=pl.ANY)


def meet(count):
    me = lax.axis_index("frame")
    barrier = pltpu.get_barrier_semaphore()
    for step in range(1, count):
        pl.semaphore_signal(
            barrier, inc=1, device_id={"frame": lax.rem(me + step, count)}, device_id_type=MESH
        )
    pl.semaphore_wait(barrier, count - 1)


def remote(source, target, send_sem, recv_sem, peer):
    return pltpu.make_async_remote_copy(
        src_ref=source,
        dst_ref=target,
        send_sem=send_sem,
        recv_sem=recv_sem,
        device_id={"frame": peer},
        device_id_type=MESH,
    )


def mod_lane(shape, width, copies):
    lane = lax.broadcasted_iota(jnp.int32, shape, 1)
    out = lane
    for at in range(1, copies):
        out = jnp.where(lane >= at * width, lane - at * width, out)
    return out


def window_tables(frames, block, nblocks, copies, offsets_ref, numer_ref):
    reach = WINDOW // block
    width = copies * frames
    frame = mod_lane((1, width), frames, copies)
    rows = []
    for back in range(reach + 1):
        start = jnp.zeros((1, width), jnp.int32)
        for w in range(nblocks):
            first = block * ((w + back) % nblocks)
            start = jnp.where(
                (frame >= first) & (frame < first + block), block * w + offsets_ref[w], start
            )
        spot = frame - start
        spot = jnp.where(spot < 0, spot + frames, spot)
        spot = jnp.where(spot < 0, spot + frames, spot)
        numer = jnp.zeros((1, width), F32)
        for j in range(WINDOW):
            numer = jnp.where(spot == j, numer_ref[j].astype(F32), numer)
        rows.append((start, numer))
    total = rows[0][1]
    for _, numer in rows[1:]:
        total = total + numer
    key = lax.broadcasted_iota(jnp.int32, (frames, width), 0)
    tables = []
    for start, numer in rows:
        spot = key - start
        spot = jnp.where(spot < 0, spot + frames, spot)
        spot = jnp.where(spot < 0, spot + frames, spot)
        tables.append((jnp.where(spot < WINDOW, 0.0, FAR).astype(F32), numer / total))
    return tables


def attend(
    count, x_ref, gain_ref, w_ref, offsets_ref, numer_ref, z_ref,
    seen_ref, q_ref, k_ref, v_ref, comb_ref, ready_ref, bias_ref, pick_ref, place_ref,
    send_sem, recv_sem, own_sem, back_send, back_recv, back_own,
):
    block, _, cells, channels = x_ref.shape
    frames = block * count
    rows = frames * cells
    nblocks = offsets_ref.shape[0]
    reach = WINDOW // block
    per = max(1, LANES // HEAD_DIM)
    me = lax.axis_index("frame")
    meet(count)
    copies = []
    for step in range(1, count):
        peer = lax.rem(me + step, count)
        copy = remote(
            x_ref.at[:, peer], seen_ref.at[me], send_sem.at[step], recv_sem.at[step], peer
        )
        copy.start()
        copies.append(copy)
    own = pltpu.make_async_copy(x_ref.at[:, me], seen_ref.at[me], own_sem)
    own.start()

    col = lax.broadcasted_iota(jnp.int32, (frames, rows), 1)
    row = lax.broadcasted_iota(jnp.int32, (frames, rows), 0)
    for p in range(cells):
        pick_ref[p * frames : (p + 1) * frames] = jnp.where(
            col == row * cells + p, 1.0, 0.0
        ).astype(BF16)
    lane = lax.broadcasted_iota(jnp.int32, (1, rows), 1)
    spot = lane * cells
    for p in range(1, cells):
        spot = jnp.where(lane >= p * frames, (lane - p * frames) * cells + p, spot)
    place_ref[...] = jnp.where(
        lax.broadcasted_iota(jnp.int32, (rows, rows), 0) == spot, 1.0, 0.0
    ).astype(BF16)
    comb_ref[...] = jnp.zeros_like(comb_ref)
    full = window_tables(frames, block, nblocks, per, offsets_ref, numer_ref)
    for back in range(reach + 1):
        bias_ref[back] = full[back][0]
    weights = [numer for _, numer in full]

    own.wait()
    for copy in copies:
        copy.wait()
    x = seen_ref[...].astype(F32).reshape(rows, channels)
    average = jnp.mean(x, axis=-1, keepdims=True)
    centered = x - average
    variance = jnp.mean(centered * centered, axis=-1, keepdims=True)
    normed = (centered * lax.rsqrt(variance + EPS) * gain_ref[...][None, :]).astype(BF16)
    normed = jnp.dot(pick_ref[...], normed, preferred_element_type=F32).astype(BF16)
    for at, ref in enumerate((q_ref, k_ref, v_ref)):
        weight = w_ref[:, at * channels : (at + 1) * channels]
        ref[...] = jnp.dot(normed, weight, preferred_element_type=F32).astype(BF16)
    scale = HEAD_DIM**-0.5
    returns = []
    for chunk, first in enumerate(range(0, HEADS, per)):
        heads = min(per, HEADS - first)
        size = heads * HEAD_DIM
        lanes = pl.ds(first * HEAD_DIM, size)
        lane = lax.broadcasted_iota(jnp.int32, (frames, size), 1)
        masks = [
            jnp.where((lane >= h * HEAD_DIM) & (lane < (h + 1) * HEAD_DIM), 1.0, 0.0).astype(BF16)
            for h in range(heads)
        ]
        width = heads * frames
        for p in range(cells):
            here = pl.ds(p * frames, frames)
            q = q_ref[here, lanes]
            k = k_ref[here, lanes]
            v = v_ref[here, lanes]
            spread = jnp.concatenate([q * m for m in masks], 0) if heads > 1 else q
            scores = (
                lax.dot_general(
                    k, spread, (((1,), (1,)), ((), ())), preferred_element_type=F32
                )
                * scale
            )
            total = jnp.zeros((frames, width), F32)
            for back in range(reach + 1):
                masked = scores + bias_ref[back, :, :width]
                expo = jnp.exp(masked - jnp.max(masked, axis=0, keepdims=True))
                level = weights[back][:, :width] / jnp.sum(expo, axis=0, keepdims=True)
                total = total + expo * level
            mixed = lax.dot_general(
                total.T.astype(BF16), v, (((1,), (0,)), ((), ())), preferred_element_type=F32
            )
            out = mixed[:frames]
            for h in range(1, heads):
                out = jnp.where(lane >= h * HEAD_DIM, mixed[h * frames : (h + 1) * frames], out)
            comb_ref[chunk, here, :size] = out.astype(BF16)
        ready_ref[chunk] = (
            jnp.dot(place_ref[...], comb_ref[chunk], preferred_element_type=F32)
            .reshape(count, block, cells, comb_ref.shape[-1])
            .astype(BF16)
        )
        for step in range(1, count):
            peer = lax.rem(me + step, count)
            copy = remote(
                ready_ref.at[chunk, peer],
                z_ref.at[chunk, :, me],
                back_send.at[chunk, step],
                back_recv.at[chunk, step],
                peer,
            )
            copy.start()
            returns.append(copy)
        own = pltpu.make_async_copy(
            ready_ref.at[chunk, me], z_ref.at[chunk, :, me], back_own.at[chunk]
        )
        own.start()
        returns.append(own)
    for copy in returns:
        copy.wait()


def attention(x, gain, w_qkv, offsets, numerators):
    block, count, cells, channels = x.shape
    rows = block * count * cells
    per = max(1, LANES // HEAD_DIM)
    chunks = -(-HEADS // per)
    wide = per * HEAD_DIM
    return pl.pallas_call(
        functools.partial(attend, count),
        out_shape=jax.ShapeDtypeStruct((chunks, block, count, cells, wide), BF16),
        in_specs=[VMEM, VMEM, VMEM, SMEM, SMEM],
        out_specs=ANY,
        scratch_shapes=[
            pltpu.VMEM((count, block, cells, channels), BF16),
            pltpu.VMEM((rows, channels), BF16),
            pltpu.VMEM((rows, channels), BF16),
            pltpu.VMEM((rows, channels), BF16),
            pltpu.VMEM((chunks, rows, wide), BF16),
            pltpu.VMEM((chunks, count, block, cells, wide), BF16),
            pltpu.VMEM((WINDOW // block + 1, block * count, per * block * count), F32),
            pltpu.VMEM((rows, rows), BF16),
            pltpu.VMEM((rows, rows), BF16),
            pltpu.SemaphoreType.DMA((count,)),
            pltpu.SemaphoreType.DMA((count,)),
            pltpu.SemaphoreType.DMA,
            pltpu.SemaphoreType.DMA((chunks, count)),
            pltpu.SemaphoreType.DMA((chunks, count)),
            pltpu.SemaphoreType.DMA((chunks,)),
        ],
        compiler_params=pltpu.CompilerParams(
            collective_id=0, has_side_effects=True, vmem_limit_bytes=40 * 2**20
        ),
    )(x, gain, w_qkv, offsets, numerators)


def group_sum(sums):
    channels = sums.shape[-1]
    size = channels // NORM_GROUPS
    row = lax.broadcasted_iota(jnp.int32, (channels, channels), 0)
    col = lax.broadcasted_iota(jnp.int32, (channels, channels), 1)
    row_group = (row.astype(F32) * (1.0 / size) + 0.5 / size).astype(jnp.int32)
    col_group = (col.astype(F32) * (1.0 / size) + 0.5 / size).astype(jnp.int32)
    same = jnp.where(row_group == col_group, 1.0, 0.0).astype(F32)
    return jnp.dot(sums, same, preferred_element_type=F32, precision=lax.Precision.HIGHEST)


def group_act(tensor, gain):
    cells, channels = tensor[0].shape
    count = cells * (channels // NORM_GROUPS)
    sums = jnp.concatenate([jnp.sum(t, axis=0, keepdims=True) for t in tensor], 0)
    average = group_sum(sums) * (1.0 / count)
    centered = [t - average[i : i + 1] for i, t in enumerate(tensor)]
    squares = jnp.concatenate([jnp.sum(c * c, axis=0, keepdims=True) for c in centered], 0)
    factor = lax.rsqrt(group_sum(squares) * (1.0 / count) + EPS) * gain
    normed = [c * factor[i : i + 1] for i, c in enumerate(centered)]
    return [v / (1.0 + jnp.exp(-v)) for v in normed]


def conv_three(acts, conv_ref, tile_rows, tile_cols):
    count = len(acts)
    lines = []
    for r in range(tile_rows):
        line = jnp.concatenate([a[r * tile_cols : (r + 1) * tile_cols] for a in acts], 0)
        length = line.shape[0]
        at = jnp.concatenate(
            [lax.broadcasted_iota(jnp.int32, (tile_cols, line.shape[1]), 0)] * count, 0
        )
        before = jnp.where(at == 0, 0.0, pltpu.roll(line, 1, 0))
        after = jnp.where(at == tile_cols - 1, 0.0, pltpu.roll(line, length - 1, 0))
        lines.append([before.astype(BF16), line.astype(BF16), after.astype(BF16)])
    outs = []
    for r in range(tile_rows):
        total = None
        for s in range(max(0, r - 1), min(tile_rows, r + 2)):
            for x in range(3):
                term = jnp.dot(lines[s][x], conv_ref[s - r + 1, x], preferred_element_type=F32)
                total = term if total is None else total + term
        outs.append(total)
    return outs


def per_frame(lines, count, tile_cols):
    return [
        jnp.concatenate([line[i * tile_cols : (i + 1) * tile_cols] for line in lines], 0)
        for i in range(count)
    ]


def residual(
    block, tile_rows, tile_cols, x_ref, z_ref, w_out_ref, gn_ref, one_ref, two_ref, step_ref, out_ref
):
    cells = tile_rows * tile_cols
    channels, wide = x_ref.shape[-1], z_ref.shape[-1]
    projected = 0.0
    for chunk in range(z_ref.shape[0]):
        first = chunk * wide
        size = min(wide, channels - first)
        projected = projected + jnp.dot(
            z_ref[chunk, :, :size], w_out_ref[first : first + size], preferred_element_type=F32
        )
    hidden = (x_ref[...].astype(F32) + projected).astype(BF16).astype(F32)
    hidden = [hidden[i * cells : (i + 1) * cells] for i in range(block)]
    acts = group_act(hidden, gn_ref[0:1])
    lines = conv_three(acts, one_ref, tile_rows, tile_cols)
    middle = per_frame([line + step_ref[...][None, :] for line in lines], block, tile_cols)
    acts = group_act(middle, gn_ref[1:2])
    lines = conv_three(acts, two_ref, tile_rows, tile_cols)
    moved = per_frame(lines, block, tile_cols)
    for i in range(block):
        out_ref[i * cells : (i + 1) * cells] = (hidden[i] + moved[i]).astype(BF16)


def resblock(x, z, w_out, gn_gain, conv_one, conv_two, step, block, tile_rows, tile_cols):
    return pl.pallas_call(
        functools.partial(residual, block, tile_rows, tile_cols),
        out_shape=jax.ShapeDtypeStruct(x.shape, BF16),
        in_specs=[VMEM] * 7,
        out_specs=VMEM,
        compiler_params=pltpu.CompilerParams(vmem_limit_bytes=60 * 2**20),
    )(x, z, w_out, gn_gain, conv_one, conv_two, step)


def body(
    latents, norm_gain, w_qkv, w_out, gn_gain, conv_one, conv_two, step_embed, offsets, numerators
):
    block, tile_rows, tile_cols, channels = latents.shape
    count = lax.axis_size("frame")
    cells = tile_rows * tile_cols // count
    split = latents.reshape(block, count, cells, channels)
    back = attention(split, norm_gain, w_qkv, offsets, numerators)
    flat = (block * tile_rows * tile_cols, channels)
    result = resblock(
        latents.reshape(flat),
        back.reshape(back.shape[0], flat[0], back.shape[-1]),
        w_out,
        gn_gain,
        conv_one,
        conv_two,
        step_embed,
        block,
        tile_rows,
        tile_cols,
    )
    return result.reshape(latents.shape)


def solution(mesh):
    return jax.shard_map(
        body,
        mesh=mesh,
        in_specs=(
            P(("groups", "frame"), None, None, None),
            P(),
            P(),
            P(),
            P(),
            P(),
            P(),
            P(),
            P("groups"),
            P(),
        ),
        out_specs=P(("groups", "frame"), None, None, None),
        check_vma=False,
    )
```

```python
import functools

import jax
import jax.numpy as jnp
from jax import lax
from jax.experimental import pallas as pl
from jax.experimental.pallas import tpu as pltpu
from jax.sharding import PartitionSpec as P

HEADS = 5
HEAD_DIM = 64
NORM_GROUPS = 32
WINDOW = 16
LANES = 128
EPS = 1e-05
FAR = -1e30
F32 = jnp.float32
BF16 = jnp.bfloat16
MESH = pl.DeviceIdType.MESH
VMEM = pl.BlockSpec(memory_space=pltpu.VMEM)
SMEM = pl.BlockSpec(memory_space=pltpu.SMEM)
ANY = pl.BlockSpec(memory_space=pl.ANY)


def meet(count):
    me = lax.axis_index("frame")
    barrier = pltpu.get_barrier_semaphore()
    for step in range(1, count):
        pl.semaphore_signal(
            barrier, inc=1, device_id={"frame": lax.rem(me + step, count)}, device_id_type=MESH
        )
    pl.semaphore_wait(barrier, count - 1)


def remote(source, target, send_sem, recv_sem, peer):
    return pltpu.make_async_remote_copy(
        src_ref=source,
        dst_ref=target,
        send_sem=send_sem,
        recv_sem=recv_sem,
        device_id={"frame": peer},
        device_id_type=MESH,
    )


def mod_lane(shape, width, copies):
    lane = lax.broadcasted_iota(jnp.int32, shape, 1)
    out = lane
    for at in range(1, copies):
        out = jnp.where(lane >= at * width, lane - at * width, out)
    return out


def window_tables(frames, block, nblocks, copies, offsets_ref, numer_ref):
    reach = WINDOW // block
    width = copies * frames
    frame = mod_lane((1, width), frames, copies)
    rows = []
    for back in range(reach + 1):
        start = jnp.zeros((1, width), jnp.int32)
        for w in range(nblocks):
            first = block * ((w + back) % nblocks)
            start = jnp.where(
                (frame >= first) & (frame < first + block), block * w + offsets_ref[w], start
            )
        spot = frame - start
        spot = jnp.where(spot < 0, spot + frames, spot)
        spot = jnp.where(spot < 0, spot + frames, spot)
        numer = jnp.zeros((1, width), F32)
        for j in range(WINDOW):
            numer = jnp.where(spot == j, numer_ref[j].astype(F32), numer)
        rows.append((start, numer))
    total = rows[0][1]
    for _, numer in rows[1:]:
        total = total + numer
    key = lax.broadcasted_iota(jnp.int32, (frames, width), 0)
    tables = []
    for start, numer in rows:
        spot = key - start
        spot = jnp.where(spot < 0, spot + frames, spot)
        spot = jnp.where(spot < 0, spot + frames, spot)
        tables.append((jnp.where(spot < WINDOW, 0.0, FAR).astype(F32), numer / total))
    return tables


def attend(
    count, x_ref, gain_ref, w_hbm, offsets_ref, numer_ref, z_ref,
    w_ref, w_sem, seen_ref, q_ref, k_ref, v_ref, comb_ref, ready_ref, bias_ref, pick_ref, place_ref,
    send_sem, recv_sem, own_sem, back_send, back_recv, back_own,
):
    block, _, cells, channels = x_ref.shape
    frames = block * count
    rows = frames * cells
    nblocks = offsets_ref.shape[0]
    reach = WINDOW // block
    per = max(1, LANES // HEAD_DIM)
    me = lax.axis_index("frame")
    meet(count)
    copies = []
    for step in range(1, count):
        peer = lax.rem(me + step, count)
        copy = remote(
            x_ref.at[:, peer], seen_ref.at[me], send_sem.at[step], recv_sem.at[step], peer
        )
        copy.start()
        copies.append(copy)
    own = pltpu.make_async_copy(x_ref.at[:, me], seen_ref.at[me], own_sem)
    own.start()
    fetch = pltpu.make_async_copy(w_hbm, w_ref, w_sem)
    fetch.start()

    col = lax.broadcasted_iota(jnp.int32, (frames, rows), 1)
    row = lax.broadcasted_iota(jnp.int32, (frames, rows), 0)
    for p in range(cells):
        pick_ref[p * frames : (p + 1) * frames] = jnp.where(
            col == row * cells + p, 1.0, 0.0
        ).astype(BF16)
    lane = lax.broadcasted_iota(jnp.int32, (1, rows), 1)
    spot = lane * cells
    for p in range(1, cells):
        spot = jnp.where(lane >= p * frames, (lane - p * frames) * cells + p, spot)
    place_ref[...] = jnp.where(
        lax.broadcasted_iota(jnp.int32, (rows, rows), 0) == spot, 1.0, 0.0
    ).astype(BF16)
    comb_ref[...] = jnp.zeros_like(comb_ref)
    full = window_tables(frames, block, nblocks, per, offsets_ref, numer_ref)
    for back in range(reach + 1):
        bias_ref[back] = full[back][0]
    weights = [numer for _, numer in full]

    fetch.wait()
    own.wait()
    for copy in copies:
        copy.wait()
    x = seen_ref[...].astype(F32).reshape(rows, channels)
    average = jnp.mean(x, axis=-1, keepdims=True)
    centered = x - average
    variance = jnp.mean(centered * centered, axis=-1, keepdims=True)
    normed = (centered * lax.rsqrt(variance + EPS) * gain_ref[...][None, :]).astype(BF16)
    normed = jnp.dot(pick_ref[...], normed, preferred_element_type=F32).astype(BF16)
    for at, ref in enumerate((q_ref, k_ref, v_ref)):
        weight = w_ref[:, at * channels : (at + 1) * channels]
        ref[...] = jnp.dot(normed, weight, preferred_element_type=F32).astype(BF16)
    scale = HEAD_DIM**-0.5
    returns = []
    for chunk, first in enumerate(range(0, HEADS, per)):
        heads = min(per, HEADS - first)
        size = heads * HEAD_DIM
        lanes = pl.ds(first * HEAD_DIM, size)
        lane = lax.broadcasted_iota(jnp.int32, (frames, size), 1)
        masks = [
            jnp.where((lane >= h * HEAD_DIM) & (lane < (h + 1) * HEAD_DIM), 1.0, 0.0).astype(BF16)
            for h in range(heads)
        ]
        width = heads * frames
        for p in range(cells):
            here = pl.ds(p * frames, frames)
            q = q_ref[here, lanes]
            k = k_ref[here, lanes]
            v = v_ref[here, lanes]
            spread = jnp.concatenate([q * m for m in masks], 0) if heads > 1 else q
            scores = (
                lax.dot_general(
                    k, spread, (((1,), (1,)), ((), ())), preferred_element_type=F32
                )
                * scale
            )
            total = jnp.zeros((frames, width), F32)
            for back in range(reach + 1):
                masked = scores + bias_ref[back, :, :width]
                expo = jnp.exp(masked - jnp.max(masked, axis=0, keepdims=True))
                level = weights[back][:, :width] / jnp.sum(expo, axis=0, keepdims=True)
                total = total + expo * level
            mixed = lax.dot_general(
                total.T.astype(BF16), v, (((1,), (0,)), ((), ())), preferred_element_type=F32
            )
            out = mixed[:frames]
            for h in range(1, heads):
                out = jnp.where(lane >= h * HEAD_DIM, mixed[h * frames : (h + 1) * frames], out)
            comb_ref[chunk, here, :size] = out.astype(BF16)
        ready_ref[chunk] = (
            jnp.dot(place_ref[...], comb_ref[chunk], preferred_element_type=F32)
            .reshape(count, block, cells, comb_ref.shape[-1])
            .astype(BF16)
        )
        for step in range(1, count):
            peer = lax.rem(me + step, count)
            copy = remote(
                ready_ref.at[chunk, peer],
                z_ref.at[chunk, :, me],
                back_send.at[chunk, step],
                back_recv.at[chunk, step],
                peer,
            )
            copy.start()
            returns.append(copy)
        own = pltpu.make_async_copy(
            ready_ref.at[chunk, me], z_ref.at[chunk, :, me], back_own.at[chunk]
        )
        own.start()
        returns.append(own)
    for copy in returns:
        copy.wait()


def attention(x, gain, w_qkv, offsets, numerators):
    block, count, cells, channels = x.shape
    rows = block * count * cells
    per = max(1, LANES // HEAD_DIM)
    chunks = -(-HEADS // per)
    wide = per * HEAD_DIM
    return pl.pallas_call(
        functools.partial(attend, count),
        out_shape=jax.ShapeDtypeStruct((chunks, block, count, cells, wide), BF16),
        in_specs=[ANY, VMEM, ANY, SMEM, SMEM],
        out_specs=ANY,
        scratch_shapes=[
            pltpu.VMEM(w_qkv.shape, BF16),
            pltpu.SemaphoreType.DMA,
            pltpu.VMEM((count, block, cells, channels), BF16),
            pltpu.VMEM((rows, channels), BF16),
            pltpu.VMEM((rows, channels), BF16),
            pltpu.VMEM((rows, channels), BF16),
            pltpu.VMEM((chunks, rows, wide), BF16),
            pltpu.VMEM((chunks, count, block, cells, wide), BF16),
            pltpu.VMEM((WINDOW // block + 1, block * count, per * block * count), F32),
            pltpu.VMEM((rows, rows), BF16),
            pltpu.VMEM((rows, rows), BF16),
            pltpu.SemaphoreType.DMA((count,)),
            pltpu.SemaphoreType.DMA((count,)),
            pltpu.SemaphoreType.DMA,
            pltpu.SemaphoreType.DMA((chunks, count)),
            pltpu.SemaphoreType.DMA((chunks, count)),
            pltpu.SemaphoreType.DMA((chunks,)),
        ],
        compiler_params=pltpu.CompilerParams(
            collective_id=0, has_side_effects=True, vmem_limit_bytes=62 * 2**20
        ),
    )(x, gain, w_qkv, offsets, numerators)


def group_sum(sums):
    channels = sums.shape[-1]
    size = channels // NORM_GROUPS
    row = lax.broadcasted_iota(jnp.int32, (channels, channels), 0)
    col = lax.broadcasted_iota(jnp.int32, (channels, channels), 1)
    row_group = (row.astype(F32) * (1.0 / size) + 0.5 / size).astype(jnp.int32)
    col_group = (col.astype(F32) * (1.0 / size) + 0.5 / size).astype(jnp.int32)
    same = jnp.where(row_group == col_group, 1.0, 0.0).astype(F32)
    return jnp.dot(sums, same, preferred_element_type=F32, precision=lax.Precision.HIGHEST)


def group_act(tensor, gain):
    cells, channels = tensor[0].shape
    count = cells * (channels // NORM_GROUPS)
    sums = jnp.concatenate([jnp.sum(t, axis=0, keepdims=True) for t in tensor], 0)
    average = group_sum(sums) * (1.0 / count)
    centered = [t - average[i : i + 1] for i, t in enumerate(tensor)]
    squares = jnp.concatenate([jnp.sum(c * c, axis=0, keepdims=True) for c in centered], 0)
    factor = lax.rsqrt(group_sum(squares) * (1.0 / count) + EPS) * gain
    normed = [c * factor[i : i + 1] for i, c in enumerate(centered)]
    return [v / (1.0 + jnp.exp(-v)) for v in normed]


def conv_three(acts, conv_ref, tile_rows, tile_cols):
    count = len(acts)
    lines = []
    for r in range(tile_rows):
        line = jnp.concatenate([a[r * tile_cols : (r + 1) * tile_cols] for a in acts], 0)
        length = line.shape[0]
        at = jnp.concatenate(
            [lax.broadcasted_iota(jnp.int32, (tile_cols, line.shape[1]), 0)] * count, 0
        )
        before = jnp.where(at == 0, 0.0, pltpu.roll(line, 1, 0))
        after = jnp.where(at == tile_cols - 1, 0.0, pltpu.roll(line, length - 1, 0))
        lines.append([before.astype(BF16), line.astype(BF16), after.astype(BF16)])
    outs = []
    for r in range(tile_rows):
        total = None
        for s in range(max(0, r - 1), min(tile_rows, r + 2)):
            for x in range(3):
                term = jnp.dot(lines[s][x], conv_ref[s - r + 1, x], preferred_element_type=F32)
                total = term if total is None else total + term
        outs.append(total)
    return outs


def per_frame(lines, count, tile_cols):
    return [
        jnp.concatenate([line[i * tile_cols : (i + 1) * tile_cols] for line in lines], 0)
        for i in range(count)
    ]


def residual(
    block, tile_rows, tile_cols, x_ref, z_ref, w_out_ref, gn_ref, one_hbm, two_hbm, step_ref, out_ref,
    one_ref, two_ref, one_sem, two_sem,
):
    cells = tile_rows * tile_cols
    first_fetch = pltpu.make_async_copy(one_hbm, one_ref, one_sem)
    first_fetch.start()
    second_fetch = pltpu.make_async_copy(two_hbm, two_ref, two_sem)
    second_fetch.start()
    channels, wide = x_ref.shape[-1], z_ref.shape[-1]
    projected = 0.0
    for chunk in range(z_ref.shape[0]):
        first = chunk * wide
        size = min(wide, channels - first)
        projected = projected + jnp.dot(
            z_ref[chunk, :, :size], w_out_ref[first : first + size], preferred_element_type=F32
        )
    hidden = (x_ref[...].astype(F32) + projected).astype(BF16).astype(F32)
    hidden = [hidden[i * cells : (i + 1) * cells] for i in range(block)]
    acts = group_act(hidden, gn_ref[0:1])
    first_fetch.wait()
    lines = conv_three(acts, one_ref, tile_rows, tile_cols)
    middle = per_frame([line + step_ref[...][None, :] for line in lines], block, tile_cols)
    acts = group_act(middle, gn_ref[1:2])
    second_fetch.wait()
    lines = conv_three(acts, two_ref, tile_rows, tile_cols)
    moved = per_frame(lines, block, tile_cols)
    for i in range(block):
        out_ref[i * cells : (i + 1) * cells] = (hidden[i] + moved[i]).astype(BF16)


def resblock(x, z, w_out, gn_gain, conv_one, conv_two, step, block, tile_rows, tile_cols):
    return pl.pallas_call(
        functools.partial(residual, block, tile_rows, tile_cols),
        out_shape=jax.ShapeDtypeStruct(x.shape, BF16),
        in_specs=[VMEM, VMEM, VMEM, VMEM, ANY, ANY, VMEM],
        out_specs=VMEM,
        scratch_shapes=[
            pltpu.VMEM(conv_one.shape, BF16),
            pltpu.VMEM(conv_two.shape, BF16),
            pltpu.SemaphoreType.DMA,
            pltpu.SemaphoreType.DMA,
        ],
        compiler_params=pltpu.CompilerParams(vmem_limit_bytes=62 * 2**20),
    )(x, z, w_out, gn_gain, conv_one, conv_two, step)


def body(
    latents, norm_gain, w_qkv, w_out, gn_gain, conv_one, conv_two, step_embed, offsets, numerators
):
    block, tile_rows, tile_cols, channels = latents.shape
    count = lax.axis_size("frame")
    cells = tile_rows * tile_cols // count
    split = latents.reshape(block, count, cells, channels)
    back = attention(split, norm_gain, w_qkv, offsets, numerators)
    flat = (block * tile_rows * tile_cols, channels)
    result = resblock(
        latents.reshape(flat),
        back.reshape(back.shape[0], flat[0], back.shape[-1]),
        w_out,
        gn_gain,
        conv_one,
        conv_two,
        step_embed,
        block,
        tile_rows,
        tile_cols,
    )
    return result.reshape(latents.shape)


def solution(mesh):
    return jax.shard_map(
        body,
        mesh=mesh,
        in_specs=(
            P(("groups", "frame"), None, None, None),
            P(),
            P(),
            P(),
            P(),
            P(),
            P(),
            P(),
            P("groups"),
            P(),
        ),
        out_specs=P(("groups", "frame"), None, None, None),
        check_vma=False,
    )
```
